32 devices in a mesh: ep: 4 (over y, x), tp: 4 (over z), dp: 2 (over core).
Axes of the slice: x: 2, y: 2, z: 4, core: 2. Of those that a mesh axis runs over, the one named last changes fastest.
Arguments:
- down_weight: bfloat16 [4, 16384, 3072], P('ep', 'tp', 'dp'), may hold values from -130 to 130
- owned_span: int32 [4, 4, 2], replicated, may hold values from 0 to 31, as said below
Outputs:
- saved_spans: bfloat16 [4, 4, 768, 16384], P('ep', 'tp', 'dp')
The draws below stay inside these ranges and needn't reach their ends.
Inputs may be any that keep to these rules, and one draw needn't show every extreme that they name: `owned_span`: block g holds rows (g % 8) * 384 onward of expert g // 8; every block is stored by exactly one device; the block at [i, j, k] has (g % 8) // 4 == k; for each k the experts of the stored blocks form a Latin square over i and j: each expert once for each i and once for each j.
All inputs are finite; a program needn't handle non-finite values.
Results may differ from the reference program's by a relative error of at most 0.001.
Values may be sent and summed in bfloat16 or wider, within the bound.
No kernel may reach another device: no remote copies, remote signals or barrier semaphores. Data moves between devices by JAX's collectives and lax.ppermute only.
A program may use at most 128 MiB of HBM per device.

```python
import jax
import jax.numpy as jnp

FF = 16384
EXPERTS = 4
SLAB = 3072
BLOCK_ROWS = 384
N_EP = 4
N_TP = 4
N_DP = 2


def permuted_rows(key, count_rows, width):
    scores = jax.random.randint(key, (count_rows, width), 0, 1 << 20) * width + jnp.arange(width, dtype=jnp.int32)[None, :]
    return jnp.argsort(scores, axis=1).astype(jnp.int32)


def draw_owned_span(key, part):
    key_list = jax.random.split(jax.random.fold_in(key, 23), 4)
    per_expert = N_TP * N_DP
    row_perm = permuted_rows(key_list[0], N_DP, N_EP)
    col_perm = permuted_rows(key_list[1], N_DP, N_TP)
    relabel = permuted_rows(key_list[2], N_DP, N_EP)
    block_perm = permuted_rows(key_list[3], N_DP * N_EP, N_TP).reshape(N_DP, N_EP, N_TP)
    summed = (row_perm[:, :, None] + col_perm[:, None, :]) % N_EP
    latin_square = jnp.take_along_axis(relabel[:, :, None], summed.reshape(N_DP, N_EP * N_TP, 1), axis=1).reshape(N_DP, N_EP, N_TP)
    replica_ids = jnp.arange(N_DP, dtype=jnp.int32)[:, None, None] + jnp.zeros((N_DP, N_EP, N_TP), jnp.int32)
    ep_ids = jnp.arange(N_EP, dtype=jnp.int32)[None, :, None] + jnp.zeros((N_DP, N_EP, N_TP), jnp.int32)
    within = replica_ids * N_TP + block_perm[replica_ids, latin_square, ep_ids]
    global_ids = latin_square * per_expert + within
    return jnp.transpose(global_ids, (1, 2, 0)).astype(jnp.int32)


def draw_down_weight(key, part):
    key_list = jax.random.split(jax.random.fold_in(key, 11), 3)
    base_draw = jnp.clip(jax.random.normal(key_list[0], (EXPERTS, FF, SLAB), jnp.float32), -4.0, 4.0)
    spread = 1.15
    row_scale = jnp.exp(jax.random.uniform(key_list[1], (SLAB,), jnp.float32, -spread, spread))
    col_scale = jnp.exp(jax.random.uniform(key_list[2], (FF,), jnp.float32, -spread, spread))
    expert_scale = jnp.power(3.0, jnp.arange(EXPERTS, dtype=jnp.float32) / max(EXPERTS - 1, 1))
    values = base_draw * expert_scale[:, None, None] * col_scale[None, :, None] * row_scale[None, None, :]
    return values.astype(jnp.bfloat16)


def setup_inputs(seed: int = 0) -> dict:
    keys = jax.random.split(jax.random.key(seed), 3)
    down_weight = draw_down_weight(jax.random.fold_in(keys[2], 71), 0)
    owned_span = draw_owned_span(jax.random.fold_in(keys[2], 71), 0)
    return {"down_weight": down_weight, "owned_span": owned_span}


def reference(down_weight, owned_span):
    per_expert = N_TP * N_DP
    saved_rows = jnp.transpose(down_weight, (0, 2, 1)).reshape(EXPERTS * per_expert, BLOCK_ROWS, FF)
    owner_list = owned_span.reshape(-1).astype(jnp.int32)
    picked = jnp.take(saved_rows, owner_list, axis=0)
    saved_spans = picked.reshape(N_EP, N_TP, N_DP * BLOCK_ROWS, FF)
    return saved_spans
```

```python
import jax
import jax.numpy as jnp
from jax import lax
from jax.experimental import pallas as pl
from jax.experimental.pallas import tpu as pltpu
from jax.sharding import PartitionSpec as P


TP_FIRST = 1
EP_FIRST = (1, 2, 4, 4, 3, 1)
ORDER = (
    "AX", "A0", "A1", "B0", "A2", "B1", "HX", "A3", "C0", "B2", "A4",
    "C1", "B3", "A5", "BX", "B4", "B5", "C2", "C3", "CX", "C4", "C5",
)
ANY = pl.BlockSpec(memory_space=pl.ANY)
SCALARS = pl.BlockSpec(memory_space=pltpu.SMEM)
PARAMS = pltpu.CompilerParams(vmem_limit_bytes=66_000_000)


def tile_of(width):
    return 256 if width % 256 == 0 else 128


def pick_rows(weight, spans, offset, width, block_rows):
    count = spans.shape[0]
    tile = tile_of(width)
    rows = weight.shape[1]

    def kernel(spans_ref, weight_ref, *refs):
        outs, turned = refs[-1 - count:-1], refs[-1]
        turned[...] = weight_ref[...].T
        for partner, out in enumerate(outs):
            start = pl.multiple_of(spans_ref[partner] * block_rows, 16)
            out[...] = turned[pl.ds(start, block_rows), :]

    return pl.pallas_call(
        kernel,
        grid_spec=pltpu.PrefetchScalarGridSpec(
            num_scalar_prefetch=1,
            grid=(width // tile,),
            in_specs=[pl.BlockSpec((tile, rows), lambda step, spans: (offset // tile + step, 0))],
            out_specs=[pl.BlockSpec((block_rows, tile), lambda step, spans: (0, step))] * count,
            scratch_shapes=[pltpu.VMEM((rows, tile), weight.dtype)],
        ),
        out_shape=[jax.ShapeDtypeStruct((block_rows, width), weight.dtype)] * count,
        compiler_params=PARAMS,
        name="pick_rows",
    )(spans, weight)


def choose(pieces, picks):
    count = len(pieces)

    def kernel(picks_ref, *refs):
        ins, outs, (held, arrive, leave) = refs[:count], refs[count:-3], refs[-3:]
        for slot in range(count):
            for source in range(count):
                @pl.when(picks_ref[slot] == source)
                def _():
                    pltpu.make_async_copy(ins[source], held.at[slot], arrive.at[slot]).start()
        for slot in range(count):
            pltpu.make_async_copy(ins[slot], held.at[slot], arrive.at[slot]).wait()
            pltpu.make_async_copy(held.at[slot], outs[slot], leave.at[slot]).start()
        for slot in range(count):
            pltpu.make_async_copy(held.at[slot], outs[slot], leave.at[slot]).wait()

    return pl.pallas_call(
        kernel,
        in_specs=[SCALARS] + [ANY] * count,
        out_specs=[ANY] * count,
        out_shape=[jax.ShapeDtypeStruct(piece.shape, piece.dtype) for piece in pieces],
        scratch_shapes=[
            pltpu.VMEM((count, *pieces[0].shape), pieces[0].dtype),
            pltpu.SemaphoreType.DMA((count,)),
            pltpu.SemaphoreType.DMA((count,)),
        ],
        compiler_params=PARAMS,
        name="choose",
    )(picks, *pieces)


def place(saved, pieces, starts, shape):
    count = len(pieces)
    width = pieces[0].shape[1]

    def kernel(starts_ref, *refs):
        ins, out, held, arrive, leave = refs[:count], *refs[-4:]
        reads, writes = [], []
        for slot in range(count):
            start = pl.multiple_of(starts_ref[slot], 128)
            reads.append(pltpu.make_async_copy(ins[slot], held.at[slot], arrive.at[slot]))
            writes.append(pltpu.make_async_copy(held.at[slot], out.at[:, pl.ds(start, width)], leave.at[slot]))
        for read in reads:
            read.start()
        for read, write in zip(reads, writes):
            read.wait()
            write.start()
        for write in writes:
            write.wait()

    return pl.pallas_call(
        kernel,
        in_specs=[SCALARS] + [ANY] * (count + len(saved)),
        out_specs=ANY,
        out_shape=jax.ShapeDtypeStruct(shape, pieces[0].dtype),
        scratch_shapes=[
            pltpu.VMEM((count, *pieces[0].shape), pieces[0].dtype),
            pltpu.SemaphoreType.DMA((count,)),
            pltpu.SemaphoreType.DMA((count,)),
        ],
        input_output_aliases={count + 1: 0} if saved else {},
        compiler_params=PARAMS,
        name="place",
    )(starts, *pieces, *saved)


def exchange(pieces, axis):
    count = len(pieces)
    return [pieces[0]] + [
        lax.ppermute(pieces[step], axis, [(index, index ^ step) for index in range(count)])
        for step in range(1, count)
    ]


def local(down_weight, owned_span):
    weight = down_weight[0]
    hidden, rows = weight.shape
    ep_count, tp_count, dp_count = (lax.axis_size(name) for name in ("ep", "tp", "dp"))
    per_expert = tp_count * dp_count
    block_rows = rows // tp_count
    me, mine, replica = (lax.axis_index(name) for name in ("ep", "tp", "dp"))
    table = lax.dynamic_index_in_dim(owned_span, replica, 2, keepdims=False)
    experts = table // per_expert
    spans = jnp.where(experts == me, table % per_expert - replica * tp_count, 0)
    steps = jnp.arange(ep_count, dtype=jnp.int32)
    spans_ep = jnp.take(jnp.sum(spans, axis=1), steps ^ me)
    spans_tp = jnp.take(jnp.sum(spans, axis=0), steps ^ mine)
    row_experts = lax.dynamic_index_in_dim(experts, me, 0, keepdims=False)
    column_experts = lax.dynamic_index_in_dim(experts, mine, 1, keepdims=False)
    picks = jnp.take(row_experts, steps ^ mine) ^ me
    picks_x = jnp.take(column_experts, steps ^ me) ^ me
    columns = (steps ^ mine) * hidden
    columns_x = (steps ^ mine ^ me ^ jnp.take(column_experts, me)) * hidden
    unit = hidden // (TP_FIRST + sum(EP_FIRST))
    shape = (block_rows, tp_count * hidden)

    offsets = {"X": 0}
    start = TP_FIRST * unit
    for chunk, share in enumerate(EP_FIRST):
        offsets[str(chunk)] = start
        start += share * unit
    moved = {}
    saved = []
    for event in ORDER:
        stage, chunk = event
        first = chunk == "X"
        if stage == "A":
            width = (TP_FIRST if first else EP_FIRST[int(chunk)]) * unit
            sent = pick_rows(weight, spans_tp if first else spans_ep, offsets[chunk], width, block_rows)
            moved[chunk] = exchange(sent, "tp" if first else "ep")
        elif stage == "H":
            moved[chunk] = exchange(moved[chunk], "ep")
        elif stage == "B":
            sent = choose(moved[chunk], picks_x if first else picks)
            moved[chunk] = exchange(sent, "ep" if first else "tp")
        else:
            places = (columns_x if first else columns) + offsets[chunk]
            saved = [place(saved, moved[chunk], places, shape)]
    return saved[0][None, None]


def solution(mesh):
    return jax.shard_map(
        local,
        mesh=mesh,
        in_specs=(P("ep", "tp", "dp"), P()),
        out_specs=P("ep", "tp", "dp", None),
        check_vma=False,
    )
```

```python
import jax
import jax.numpy as jnp
from jax import lax
from jax.experimental import pallas as pl
from jax.experimental.pallas import tpu as pltpu
from jax.sharding import PartitionSpec as P


SHARES = {"X": 1, "Y": 3, "0": 2, "1": 4, "2": 8, "3": 8, "4": 4, "5": 2}
TP_FIRST = "XY"
ORDER = (
    "AX", "AY", "A0", "A1", "B0", "HX", "A2", "B1", "HY", "A3", "C0", "B2", "A4",
    "BX", "C1", "BY", "A5", "B3", "B4", "B5", "C2", "CX", "CY", "C3", "C4", "C5",
)
ANY = pl.BlockSpec(memory_space=pl.ANY)
SCALARS = pl.BlockSpec(memory_space=pltpu.SMEM)
PARAMS = pltpu.CompilerParams(vmem_limit_bytes=66_000_000)


def tile_of(offset, width):
    return 256 if offset % 256 == 0 and width % 256 == 0 else 128


def spread(hidden):
    total = sum(SHARES.values())
    columns = hidden // 128
    edges, done = [0], 0
    for share in SHARES.values():
        done += share
        edges.append(-(-done * columns // total) * 128)
    return {chunk: (low, high - low) for chunk, low, high in zip(SHARES, edges, edges[1:])}


def axis_of(stage, chunk):
    if stage == "A":
        return "tp" if chunk in TP_FIRST else "ep"
    if stage == "B":
        return "ep" if chunk in TP_FIRST else "tp"
    return "ep" if stage == "H" else None


def steps_of(axis, count):
    return range(count - 1, 0, -1) if axis == "tp" else range(1, count)


def pick_rows(weight, spans, offset, width, block_rows):
    count = spans.shape[0]
    tile = tile_of(offset, width)
    rows = weight.shape[1]

    def kernel(spans_ref, weight_ref, *refs):
        outs, turned = refs[-1 - count:-1], refs[-1]
        turned[...] = weight_ref[...].T
        for partner, out in enumerate(outs):
            start = pl.multiple_of(spans_ref[partner] * block_rows, 16)
            out[...] = turned[pl.ds(start, block_rows), :]

    return pl.pallas_call(
        kernel,
        grid_spec=pltpu.PrefetchScalarGridSpec(
            num_scalar_prefetch=1,
            grid=(width // tile,),
            in_specs=[pl.BlockSpec((tile, rows), lambda step, spans: (offset // tile + step, 0))],
            out_specs=[pl.BlockSpec((block_rows, tile), lambda step, spans: (0, step))] * count,
            scratch_shapes=[pltpu.VMEM((rows, tile), weight.dtype)],
        ),
        out_shape=[jax.ShapeDtypeStruct((block_rows, width), weight.dtype)] * count,
        compiler_params=PARAMS,
        name="pick_rows",
    )(spans, weight)


def choose(pieces, picks):
    count = len(pieces)

    def kernel(picks_ref, *refs):
        ins, outs, (held, arrive, leave) = refs[:count], refs[count:-3], refs[-3:]
        for slot in range(count):
            for source in range(count):
                @pl.when(picks_ref[slot] == source)
                def _():
                    pltpu.make_async_copy(ins[source], held.at[slot], arrive.at[slot]).start()
        for slot in range(count):
            pltpu.make_async_copy(ins[slot], held.at[slot], arrive.at[slot]).wait()
            pltpu.make_async_copy(held.at[slot], outs[slot], leave.at[slot]).start()
        for slot in range(count):
            pltpu.make_async_copy(held.at[slot], outs[slot], leave.at[slot]).wait()

    return pl.pallas_call(
        kernel,
        in_specs=[SCALARS] + [ANY] * count,
        out_specs=[ANY] * count,
        out_shape=[jax.ShapeDtypeStruct(piece.shape, piece.dtype) for piece in pieces],
        scratch_shapes=[
            pltpu.VMEM((count, *pieces[0].shape), pieces[0].dtype),
            pltpu.SemaphoreType.DMA((count,)),
            pltpu.SemaphoreType.DMA((count,)),
        ],
        compiler_params=PARAMS,
        name="choose",
    )(picks, *pieces)


def place(saved, pieces, starts, shape):
    count = len(pieces)
    width = pieces[0].shape[1]

    def kernel(starts_ref, *refs):
        ins, out, held, arrive, leave = refs[:count], *refs[-4:]
        reads, writes = [], []
        for slot in range(count):
            start = pl.multiple_of(starts_ref[slot], 128)
            reads.append(pltpu.make_async_copy(ins[slot], held.at[slot], arrive.at[slot]))
            writes.append(pltpu.make_async_copy(held.at[slot], out.at[:, pl.ds(start, width)], leave.at[slot]))
        for read in reads:
            read.start()
        for read, write in zip(reads, writes):
            read.wait()
            write.start()
        for write in writes:
            write.wait()

    return pl.pallas_call(
        kernel,
        in_specs=[SCALARS] + [ANY] * (count + len(saved)),
        out_specs=ANY,
        out_shape=jax.ShapeDtypeStruct(shape, pieces[0].dtype),
        scratch_shapes=[
            pltpu.VMEM((count, *pieces[0].shape), pieces[0].dtype),
            pltpu.SemaphoreType.DMA((count,)),
            pltpu.SemaphoreType.DMA((count,)),
        ],
        input_output_aliases={count + 1: 0} if saved else {},
        compiler_params=PARAMS,
        name="place",
    )(starts, *pieces, *saved)


def exchange(pieces, axis):
    count = len(pieces)
    moved = {0: pieces[0]}
    for step in steps_of(axis, count):
        moved[step] = lax.ppermute(pieces[step], axis, [(index, index ^ step) for index in range(count)])
    return [moved[step] for step in range(count)]


def local(down_weight, owned_span):
    weight = down_weight[0]
    hidden, rows = weight.shape
    ep_count, tp_count, dp_count = (lax.axis_size(name) for name in ("ep", "tp", "dp"))
    per_expert = tp_count * dp_count
    block_rows = rows // tp_count
    me, mine, replica = (lax.axis_index(name) for name in ("ep", "tp", "dp"))
    table = lax.dynamic_index_in_dim(owned_span, replica, 2, keepdims=False)
    experts = table // per_expert
    spans = jnp.where(experts == me, table % per_expert - replica * tp_count, 0)
    steps = jnp.arange(ep_count, dtype=jnp.int32)
    spans_ep = jnp.take(jnp.sum(spans, axis=1), steps ^ me)
    spans_tp = jnp.take(jnp.sum(spans, axis=0), steps ^ mine)
    row_experts = lax.dynamic_index_in_dim(experts, me, 0, keepdims=False)
    column_experts = lax.dynamic_index_in_dim(experts, mine, 1, keepdims=False)
    picks = jnp.take(row_experts, steps ^ mine) ^ me
    picks_x = jnp.take(column_experts, steps ^ me) ^ me
    columns = (steps ^ mine) * hidden
    columns_x = (steps ^ mine ^ me ^ jnp.take(column_experts, me)) * hidden
    shape = (block_rows, tp_count * hidden)
    chunks = spread(hidden)

    moved = {}
    saved = []
    for stage, chunk in ORDER:
        first = chunk in TP_FIRST
        offset, width = chunks[chunk]
        if stage == "A":
            sent = pick_rows(weight, spans_tp if first else spans_ep, offset, width, block_rows)
        elif stage == "H":
            sent = moved[chunk]
        elif stage == "B":
            sent = choose(moved[chunk], picks_x if first else picks)
        else:
            places = (columns_x if first else columns) + offset
            saved = [place(saved, moved[chunk], places, shape)]
            continue
        moved[chunk] = exchange(sent, axis_of(stage, chunk))
    return saved[0][None, None]


def solution(mesh):
    return jax.shard_map(
        local,
        mesh=mesh,
        in_specs=(P("ep", "tp", "dp"), P()),
        out_specs=P("ep", "tp", "dp", None),
        check_vma=False,
    )
```

```python
import jax
import jax.numpy as jnp
from jax import lax
from jax.experimental import pallas as pl
from jax.experimental.pallas import tpu as pltpu
from jax.sharding import PartitionSpec as P


SHARES = {"X": 1, "Y": 3, "0": 2, "1": 4, "2": 8, "3": 8, "4": 4, "5": 2}
TP_FIRST = "XY"
ORDER = (
    "AX", "AY", "A0", "A1", "B0", "HX", "A2", "B1", "HY", "A3", "C0", "B2", "A4",
    "BX", "C1", "BY", "A5", "B3", "B4", "B5", "C2", "CX", "CY", "C3", "C4", "C5",
)
ANY = pl.BlockSpec(memory_space=pl.ANY)
SCALARS = pl.BlockSpec(memory_space=pltpu.SMEM)
WHOLE = pl.BlockSpec(memory_space=pltpu.VMEM)


def position():
    return lax.axis_index("ep"), lax.axis_index("tp"), lax.axis_index("dp")


def expert_of(owned, row, column, replica, sizes):
    return lax.div(owned[row, replica, column], sizes[1] * sizes[2])


def span_of(owned, expert, row, column, replica, sizes):
    span = owned[row, replica, column] - (expert * sizes[2] + replica) * sizes[1]
    return jnp.where((span >= 0) & (span < sizes[1]), span, 0)


def tile_of(offset, width):
    return 256 if offset % 256 == 0 and width % 256 == 0 else 128


def spread(hidden):
    total = sum(SHARES.values())
    columns = hidden // 128
    edges, done = [0], 0
    for share in SHARES.values():
        done += share
        edges.append(-(-done * columns // total) * 128)
    return {chunk: (low, high - low) for chunk, low, high in zip(SHARES, edges, edges[1:])}


def axis_of(stage, chunk):
    if stage == "A":
        return "tp" if chunk in TP_FIRST else "ep"
    if stage == "B":
        return "ep" if chunk in TP_FIRST else "tp"
    return "ep" if stage == "H" else None


def steps_of(axis, count):
    return range(count - 1, 0, -1) if axis == "tp" else range(1, count)


def pick_rows(weight, owned, sizes, first, offset, width):
    count = sizes[1]
    tile = tile_of(offset, width)
    rows = weight.shape[1]
    block_rows = rows // count

    def kernel(owned_ref, weight_ref, *refs):
        outs, turned = refs[:-1], refs[-1]
        me, mine, replica = position()
        turned[...] = weight_ref[...].T
        for step, out in enumerate(outs):
            owners = [(line, mine ^ step) if first else (me ^ step, line) for line in range(count)]
            span = sum(span_of(owned_ref, me, row, column, replica, sizes) for row, column in owners)
            out[...] = turned[pl.ds(pl.multiple_of(span * block_rows, 16), block_rows), :]

    return pl.pallas_call(
        kernel,
        grid=(width // tile,),
        in_specs=[SCALARS, pl.BlockSpec((tile, rows), lambda step: (offset // tile + step, 0))],
        out_specs=[pl.BlockSpec((block_rows, tile), lambda step: (0, step))] * count,
        out_shape=[jax.ShapeDtypeStruct((block_rows, width), weight.dtype)] * count,
        scratch_shapes=[pltpu.VMEM((rows, tile), weight.dtype)],
        name="pick_rows",
    )(owned, weight)


def choose(pieces, owned, sizes, first):
    count = len(pieces)

    def kernel(owned_ref, *refs):
        ins, outs = refs[:count], refs[count:]
        me, mine, replica = position()
        for step in range(count):
            row, column = (me ^ step, mine) if first else (me, mine ^ step)
            pick = expert_of(owned_ref, row, column, replica, sizes) ^ me
            for source in range(count):
                @pl.when(pick == source)
                def _():
                    outs[step][...] = ins[source][...]

    return pl.pallas_call(
        kernel,
        in_specs=[SCALARS] + [WHOLE] * count,
        out_specs=[WHOLE] * count,
        out_shape=[jax.ShapeDtypeStruct(piece.shape, piece.dtype) for piece in pieces],
        name="choose",
    )(owned, *pieces)


def place(saved, pieces, owned, sizes, first, offset, hidden):
    count = len(pieces)
    block_rows, width = pieces[0].shape

    def kernel(owned_ref, *refs):
        ins, out, sems = refs[:count], refs[-2], refs[-1]
        me, mine, replica = position()
        turn = mine ^ me ^ expert_of(owned_ref, me, mine, replica, sizes) if first else mine
        copies = []
        for step in range(count):
            start = pl.multiple_of((turn ^ step) * hidden + offset, 128)
            copies.append(pltpu.make_async_copy(ins[step], out.at[:, pl.ds(start, width)], sems.at[step]))
        for copy in copies:
            copy.start()
        for copy in copies:
            copy.wait()

    return pl.pallas_call(
        kernel,
        in_specs=[SCALARS] + [WHOLE] * count + [ANY] * len(saved),
        out_specs=ANY,
        out_shape=jax.ShapeDtypeStruct((block_rows, count * hidden), pieces[0].dtype),
        scratch_shapes=[pltpu.SemaphoreType.DMA((count,))],
        input_output_aliases={count + 1: 0} if saved else {},
        name="place",
    )(owned, *pieces, *saved)


def exchange(pieces, axis):
    count = len(pieces)
    moved = {0: pieces[0]}
    for step in steps_of(axis, count):
        moved[step] = lax.ppermute(pieces[step], axis, [(index, index ^ step) for index in range(count)])
    return [moved[step] for step in range(count)]


def local(down_weight, owned_span):
    weight = down_weight[0]
    hidden = weight.shape[0]
    owned = jnp.transpose(owned_span, (0, 2, 1))
    sizes = tuple(lax.axis_size(name) for name in ("ep", "tp", "dp"))
    chunks = spread(hidden)

    moved = {}
    saved = []
    for stage, chunk in ORDER:
        first = chunk in TP_FIRST
        offset, width = chunks[chunk]
        if stage == "A":
            sent = pick_rows(weight, owned, sizes, first, offset, width)
        elif stage == "H":
            sent = moved[chunk]
        elif stage == "B":
            sent = choose(moved[chunk], owned, sizes, first)
        else:
            saved = [place(saved, moved[chunk], owned, sizes, first, offset, hidden)]
            continue
        moved[chunk] = exchange(sent, axis_of(stage, chunk))
    return saved[0][None, None]


def solution(mesh):
    return jax.shard_map(
        local,
        mesh=mesh,
        in_specs=(P("ep", "tp", "dp"), P()),
        out_specs=P("ep", "tp", "dp", None),
        check_vma=False,
    )
```

```python
import jax
import jax.numpy as jnp
from jax import lax
from jax.experimental import pallas as pl
from jax.experimental.pallas import tpu as pltpu
from jax.sharding import PartitionSpec as P


SHARES = {"X": 1, "Y": 3, "0": 2, "1": 4, "2": 8, "3": 8, "4": 4, "5": 2}
TP_FIRST = "XY"
ORDER = (
    "AX", "AY", "A0", "A1", "B0", "HX", "A2", "B1", "HY", "A3", "C0", "B2", "A4",
    "BX", "C1", "BY", "A5", "B3", "B4", "B5", "C2", "CX", "CY", "C3", "C4", "C5",
)
ANY = pl.BlockSpec(memory_space=pl.ANY)
SCALARS = pl.BlockSpec(memory_space=pltpu.SMEM)
PARAMS = pltpu.CompilerParams(vmem_limit_bytes=8 << 20)
WHOLE = pl.BlockSpec(memory_space=pltpu.VMEM)


def position():
    return lax.axis_index("ep"), lax.axis_index("tp"), lax.axis_index("dp")


def expert_of(owned, row, column, replica, sizes):
    return lax.div(owned[row, replica, column], sizes[1] * sizes[2])


def span_of(owned, expert, row, column, replica, sizes):
    span = owned[row, replica, column] - (expert * sizes[2] + replica) * sizes[1]
    return jnp.where((span >= 0) & (span < sizes[1]), span, 0)


def tile_of(offset, width):
    return 256 if offset % 256 == 0 and width % 256 == 0 else 128


def spread(hidden):
    total = sum(SHARES.values())
    columns = hidden // 128
    edges, done = [0], 0
    for share in SHARES.values():
        done += share
        edges.append(-(-done * columns // total) * 128)
    return {chunk: (low, high - low) for chunk, low, high in zip(SHARES, edges, edges[1:])}


def axis_of(stage, chunk):
    if stage == "A":
        return "tp" if chunk in TP_FIRST else "ep"
    if stage == "B":
        return "ep" if chunk in TP_FIRST else "tp"
    return "ep" if stage == "H" else None


def steps_of(axis, count):
    return range(count - 1, 0, -1) if axis == "tp" else range(1, count)


def in_vmem(pieces):
    return [pltpu.with_memory_space_constraint(piece, pltpu.VMEM) for piece in pieces]


def pick_rows(weight, owned, sizes, first, offset, width):
    count = sizes[1]
    tile = tile_of(offset, width)
    rows = weight.shape[1]
    block_rows = rows // count

    def kernel(owned_ref, weight_ref, *refs):
        outs, turned = refs[:-1], refs[-1]
        me, mine, replica = position()
        turned[...] = weight_ref[...].T
        columns = pl.ds(pl.multiple_of(pl.program_id(0) * tile, 128), tile)
        for step, out in enumerate(outs):
            owners = [(line, mine ^ step) if first else (me ^ step, line) for line in range(count)]
            span = sum(span_of(owned_ref, me, row, column, replica, sizes) for row, column in owners)
            out[:, columns] = turned[pl.ds(pl.multiple_of(span * block_rows, 16), block_rows), :]

    return pl.pallas_call(
        kernel,
        grid=(width // tile,),
        in_specs=[SCALARS, pl.BlockSpec((tile, rows), lambda step: (offset // tile + step, 0))],
        out_specs=[WHOLE] * count,
        out_shape=[pltpu.VMEM((block_rows, width), weight.dtype)] * count,
        scratch_shapes=[pltpu.VMEM((rows, tile), weight.dtype)],
        compiler_params=PARAMS,
        name="pick_rows",
    )(owned, weight)


def choose(pieces, owned, sizes, first):
    count = len(pieces)

    def kernel(owned_ref, *refs):
        ins, outs = refs[:count], refs[count:]
        me, mine, replica = position()
        for step in range(count):
            row, column = (me ^ step, mine) if first else (me, mine ^ step)
            pick = expert_of(owned_ref, row, column, replica, sizes) ^ me
            for source in range(count):
                @pl.when(pick == source)
                def _():
                    outs[step][...] = ins[source][...]

    return pl.pallas_call(
        kernel,
        in_specs=[SCALARS] + [WHOLE] * count,
        out_specs=[WHOLE] * count,
        out_shape=[pltpu.VMEM(piece.shape, piece.dtype) for piece in pieces],
        compiler_params=PARAMS,
        name="choose",
    )(owned, *in_vmem(pieces))


def place(saved, pieces, owned, sizes, first, offset, hidden):
    count = len(pieces)
    block_rows, width = pieces[0].shape

    def kernel(owned_ref, *refs):
        ins, out, sems = refs[:count], refs[-2], refs[-1]
        me, mine, replica = position()
        turn = mine ^ me ^ expert_of(owned_ref, me, mine, replica, sizes) if first else mine
        copies = []
        for step in range(count):
            start = pl.multiple_of((turn ^ step) * hidden + offset, 128)
            copies.append(pltpu.make_async_copy(ins[step], out.at[:, pl.ds(start, width)], sems.at[step]))
        for copy in copies:
            copy.start()
        for copy in copies:
            copy.wait()

    return pl.pallas_call(
        kernel,
        in_specs=[SCALARS] + [WHOLE] * count + [ANY] * len(saved),
        out_specs=ANY,
        out_shape=jax.ShapeDtypeStruct((block_rows, count * hidden), pieces[0].dtype),
        scratch_shapes=[pltpu.SemaphoreType.DMA((count,))],
        input_output_aliases={count + 1: 0} if saved else {},
        compiler_params=PARAMS,
        name="place",
    )(owned, *in_vmem(pieces), *saved)


def exchange(pieces, axis):
    count = len(pieces)
    moved = {0: pieces[0]}
    for step in steps_of(axis, count):
        moved[step] = lax.ppermute(pieces[step], axis, [(index, index ^ step) for index in range(count)])
    return [moved[step] for step in range(count)]


def local(down_weight, owned_span):
    weight = pltpu.with_memory_space_constraint(down_weight[0], pltpu.HBM)
    hidden = weight.shape[0]
    owned = pltpu.with_memory_space_constraint(jnp.transpose(owned_span, (0, 2, 1)), pltpu.HBM)
    sizes = tuple(lax.axis_size(name) for name in ("ep", "tp", "dp"))
    chunks = spread(hidden)

    moved = {}
    saved = []
    for stage, chunk in ORDER:
        first = chunk in TP_FIRST
        offset, width = chunks[chunk]
        if stage == "A":
            sent = pick_rows(weight, owned, sizes, first, offset, width)
        elif stage == "H":
            sent = moved[chunk]
        elif stage == "B":
            sent = choose(moved[chunk], owned, sizes, first)
        else:
            saved = [place(saved, moved[chunk], owned, sizes, first, offset, hidden)]
            continue
        moved[chunk] = exchange(sent, axis_of(stage, chunk))
    return saved[0][None, None]


def solution(mesh):
    return jax.shard_map(
        local,
        mesh=mesh,
        in_specs=(P("ep", "tp", "dp"), P()),
        out_specs=P("ep", "tp", "dp", None),
        check_vma=False,
    )
```

```python
import jax
import jax.numpy as jnp
from jax import lax
from jax.experimental import pallas as pl
from jax.experimental.pallas import tpu as pltpu
from jax.sharding import PartitionSpec as P


SHARES = {"X": 1, "Y": 3, "0": 2, "1": 4, "2": 8, "3": 8, "4": 4, "5": 2}
TP_FIRST = "XY"
ORDER = (
    "AX", "AY", "A0", "A1", "B0", "HX", "A2", "B1", "HY", "A3", "C0", "B2", "A4",
    "BX", "C1", "BY", "A5", "B3", "B4", "B5", "C2", "CX", "CY", "C3", "C4", "C5",
)
ANY = pl.BlockSpec(memory_space=pl.ANY)
SCALARS = pl.BlockSpec(memory_space=pltpu.SMEM)
PARAMS = pltpu.CompilerParams(vmem_limit_bytes=8 << 20)
WHOLE = pl.BlockSpec(memory_space=pltpu.VMEM)


def position():
    return lax.axis_index("ep"), lax.axis_index("tp"), lax.axis_index("dp")


def expert_of(owned, row, column, replica, sizes):
    return lax.div(owned[row, replica, column], sizes[1] * sizes[2])


def span_of(owned, expert, row, column, replica, sizes):
    span = owned[row, replica, column] - (expert * sizes[2] + replica) * sizes[1]
    return jnp.where((span >= 0) & (span < sizes[1]), span, 0)


def tile_of(offset, width):
    return 256 if offset % 256 == 0 and width % 256 == 0 else 128


def spread(hidden):
    total = sum(SHARES.values())
    columns = hidden // 128
    edges, done = [0], 0
    for left, share in zip(reversed(range(len(SHARES))), SHARES.values()):
        done += share
        edges.append(max(edges[-1] + 1, min(done * columns // total, columns - left)))
    return {chunk: (low * 128, (high - low) * 128) for chunk, low, high in zip(SHARES, edges, edges[1:])}


def axis_of(stage, chunk):
    if stage == "A":
        return "tp" if chunk in TP_FIRST else "ep"
    if stage == "B":
        return "ep" if chunk in TP_FIRST else "tp"
    return "ep" if stage == "H" else None


def steps_of(axis, count, chunk):
    steps = list(range(1, count))
    if axis == "tp" and chunk != ORDER[-1][1]:
        steps.insert(0, steps.pop(count // 2 - 1))
    return steps


def partner_of(axis, index, step, count):
    if axis == "ep":
        return index ^ abs(step)
    rank = index
    shift = 1
    while shift < count:
        rank = rank ^ (rank >> shift)
        shift *= 2
    rank = (rank + step) & (count - 1)
    return rank ^ (rank >> 1)


def in_vmem(pieces):
    return [pltpu.with_memory_space_constraint(piece, pltpu.VMEM) for piece in pieces]


def pick_rows(weight, owned, sizes, first, offset, width):
    count = sizes[1]
    tile = tile_of(offset, width)
    rows = weight.shape[1]
    block_rows = rows // count

    def kernel(owned_ref, weight_ref, *refs):
        outs, turned = refs[:-1], refs[-1]
        me, mine, replica = position()
        turned[...] = weight_ref[...].T
        columns = pl.ds(pl.multiple_of(pl.program_id(0) * tile, 128), tile)
        for step, out in enumerate(outs):
            row, column = me ^ step, partner_of("tp", mine, step, count)
            owners = [(line, column) if first else (row, line) for line in range(count)]
            span = sum(span_of(owned_ref, me, row, column, replica, sizes) for row, column in owners)
            out[:, columns] = turned[pl.ds(pl.multiple_of(span * block_rows, 16), block_rows), :]

    return pl.pallas_call(
        kernel,
        grid=(width // tile,),
        in_specs=[SCALARS, pl.BlockSpec((tile, rows), lambda step: (offset // tile + step, 0))],
        out_specs=[WHOLE] * count,
        out_shape=[pltpu.VMEM((block_rows, width), weight.dtype)] * count,
        scratch_shapes=[pltpu.VMEM((rows, tile), weight.dtype)],
        compiler_params=PARAMS,
        name="pick_rows",
    )(owned, weight)


def choose(pieces, owned, sizes, first):
    count = len(pieces)

    def kernel(owned_ref, *refs):
        ins, outs = refs[:count], refs[count:]
        me, mine, replica = position()
        for step in range(count):
            row, column = (me ^ step, mine) if first else (me, partner_of("tp", mine, step, count))
            pick = expert_of(owned_ref, row, column, replica, sizes) ^ me
            for source in range(count):
                @pl.when(pick == source)
                def _():
                    outs[step][...] = ins[source][...]

    return pl.pallas_call(
        kernel,
        in_specs=[SCALARS] + [WHOLE] * count,
        out_specs=[WHOLE] * count,
        out_shape=[pltpu.VMEM(piece.shape, piece.dtype) for piece in pieces],
        compiler_params=PARAMS,
        name="choose",
    )(owned, *in_vmem(pieces))


def place(saved, pieces, owned, sizes, first, offset, hidden):
    count = len(pieces)
    block_rows, width = pieces[0].shape

    table = [owned] if first else []

    def kernel(*refs):
        ins, out, sems = refs[len(table):len(table) + count], refs[-2], refs[-1]
        me, mine, replica = position()
        copies = []
        for step in range(count):
            crossed = step
            if first:
                crossed = me ^ step ^ expert_of(refs[0], me, mine, replica, sizes)
            origin = partner_of("tp", mine, -crossed, count)
            start = pl.multiple_of(origin * hidden + offset, 128)
            copies.append(pltpu.make_async_copy(ins[step], out.at[:, pl.ds(start, width)], sems.at[step]))
        for copy in copies:
            copy.start()
        for copy in copies:
            copy.wait()

    return pl.pallas_call(
        kernel,
        in_specs=[SCALARS] * len(table) + [WHOLE] * count + [ANY] * len(saved),
        out_specs=ANY,
        out_shape=jax.ShapeDtypeStruct((block_rows, count * hidden), pieces[0].dtype),
        scratch_shapes=[pltpu.SemaphoreType.DMA((count,))],
        input_output_aliases={len(table) + count: 0} if saved else {},
        compiler_params=PARAMS,
        name="place",
    )(*table, *in_vmem(pieces), *saved)


def exchange(pieces, axis, chunk):
    count = len(pieces)
    moved = {0: pieces[0]}
    for step in steps_of(axis, count, chunk):
        pairs = [(index, partner_of(axis, index, step, count)) for index in range(count)]
        moved[step] = lax.ppermute(pieces[step], axis, pairs)
    return [moved[step] for step in range(count)]


def local(down_weight, owned_span):
    weight = pltpu.with_memory_space_constraint(down_weight[0], pltpu.HBM)
    hidden = weight.shape[0]
    owned = pltpu.with_memory_space_constraint(jnp.transpose(owned_span, (0, 2, 1)), pltpu.HBM)
    sizes = tuple(lax.axis_size(name) for name in ("ep", "tp", "dp"))
    chunks = spread(hidden)

    moved = {}
    saved = []
    for stage, chunk in ORDER:
        first = chunk in TP_FIRST
        offset, width = chunks[chunk]
        if stage == "A":
            sent = pick_rows(weight, owned, sizes, first, offset, width)
        elif stage == "H":
            sent = moved[chunk]
        elif stage == "B":
            sent = choose(moved[chunk], owned, sizes, first)
        else:
            saved = [place(saved, moved[chunk], owned, sizes, first, offset, hidden)]
            continue
        moved[chunk] = exchange(sent, axis_of(stage, chunk), chunk)
    return saved[0][None, None]


def solution(mesh):
    return jax.shard_map(
        local,
        mesh=mesh,
        in_specs=(P("ep", "tp", "dp"), P()),
        out_specs=P("ep", "tp", "dp", None),
        check_vma=False,
    )
```

```python
import jax
import jax.numpy as jnp
from jax import lax
from jax.experimental import pallas as pl
from jax.experimental.pallas import tpu as pltpu
from jax.sharding import PartitionSpec as P


SHARES = {"X": 1, "Y": 3, "0": 2, "1": 4, "2": 6, "3": 8, "4": 6, "5": 2}
TP_FIRST = "XY"
ORDER = (
    "AX", "AY", "A0", "A1", "B0", "HX", "A2", "B1", "HY", "A3", "C0", "B2", "A4",
    "BX", "C1", "BY", "A5", "B3", "B4", "B5", "C2", "CX", "CY", "C3", "C4", "C5",
)
WORTH_CHUNKS = 1 << 19
ANY = pl.BlockSpec(memory_space=pl.ANY)
SCALARS = pl.BlockSpec(memory_space=pltpu.SMEM)
PARAMS = pltpu.CompilerParams(vmem_limit_bytes=8 << 20)
WHOLE = pl.BlockSpec(memory_space=pltpu.VMEM)


def position():
    return lax.axis_index("ep"), lax.axis_index("tp"), lax.axis_index("dp")


def expert_of(owned, row, column, replica, sizes):
    return lax.div(owned[row, replica, column], sizes[1] * sizes[2])


def span_of(owned, expert, row, column, replica, sizes):
    span = owned[row, replica, column] - (expert * sizes[2] + replica) * sizes[1]
    return jnp.where((span >= 0) & (span < sizes[1]), span, 0)


def tile_of(offset, width):
    return 256 if offset % 256 == 0 and width % 256 == 0 else 128


def plan_of(hidden, block_rows):
    columns = hidden // 128
    if hidden * block_rows < WORTH_CHUNKS or columns < len(SHARES):
        return {"0": (0, hidden)}, ("A0", "B0", "C0")
    total = sum(SHARES.values())
    edges, done = [0], 0
    for left, share in zip(reversed(range(len(SHARES))), SHARES.values()):
        done += share
        edges.append(max(edges[-1] + 1, min(done * columns // total, columns - left)))
    return {chunk: (low * 128, (high - low) * 128) for chunk, low, high in zip(SHARES, edges, edges[1:])}, ORDER


def axis_of(stage, chunk):
    if stage == "A":
        return "tp" if chunk in TP_FIRST else "ep"
    if stage == "B":
        return "ep" if chunk in TP_FIRST else "tp"
    return "ep" if stage == "H" else None


def steps_of(axis, count, last):
    steps = list(range(1, count))
    if axis == "tp" and not last:
        steps.insert(0, steps.pop(count // 2 - 1))
    return steps


def partner_of(axis, index, step, count):
    if axis == "ep":
        return index ^ abs(step)
    rank = index
    shift = 1
    while shift < count:
        rank = rank ^ (rank >> shift)
        shift *= 2
    rank = (rank + step) & (count - 1)
    return rank ^ (rank >> 1)


def in_vmem(pieces):
    return [pltpu.with_memory_space_constraint(piece, pltpu.VMEM) for piece in pieces]


def pick_rows(weight, owned, sizes, first, offset, width):
    count = sizes[1]
    tile = tile_of(offset, width)
    rows = weight.shape[1]
    block_rows = rows // count

    def kernel(owned_ref, weight_ref, *refs):
        outs, turned = refs[:-1], refs[-1]
        me, mine, replica = position()
        turned[...] = weight_ref[...].T
        columns = pl.ds(pl.multiple_of(pl.program_id(0) * tile, 128), tile)
        for step, out in enumerate(outs):
            row, column = me ^ step, partner_of("tp", mine, step, count)
            owners = [(line, column) if first else (row, line) for line in range(count)]
            span = sum(span_of(owned_ref, me, row, column, replica, sizes) for row, column in owners)
            out[:, columns] = turned[pl.ds(pl.multiple_of(span * block_rows, 16), block_rows), :]

    return pl.pallas_call(
        kernel,
        grid=(width // tile,),
        in_specs=[SCALARS, pl.BlockSpec((tile, rows), lambda step: (offset // tile + step, 0))],
        out_specs=[WHOLE] * count,
        out_shape=[pltpu.VMEM((block_rows, width), weight.dtype)] * count,
        scratch_shapes=[pltpu.VMEM((rows, tile), weight.dtype)],
        compiler_params=PARAMS,
        name="pick_rows",
    )(owned, weight)


def choose(pieces, owned, sizes, first):
    count = len(pieces)

    def kernel(owned_ref, *refs):
        ins, outs = refs[:count], refs[count:]
        me, mine, replica = position()
        for step in range(count):
            row, column = (me ^ step, mine) if first else (me, partner_of("tp", mine, step, count))
            pick = expert_of(owned_ref, row, column, replica, sizes) ^ me
            for source in range(count):
                @pl.when(pick == source)
                def _():
                    outs[step][...] = ins[source][...]

    return pl.pallas_call(
        kernel,
        in_specs=[SCALARS] + [WHOLE] * count,
        out_specs=[WHOLE] * count,
        out_shape=[pltpu.VMEM(piece.shape, piece.dtype) for piece in pieces],
        compiler_params=PARAMS,
        name="choose",
    )(owned, *in_vmem(pieces))


def place(saved, pieces, owned, sizes, first, offset, hidden):
    count = len(pieces)
    block_rows, width = pieces[0].shape

    table = [owned] if first else []

    def kernel(*refs):
        ins, out, sems = refs[len(table):len(table) + count], refs[-2], refs[-1]
        me, mine, replica = position()
        copies = []
        for step in range(count):
            crossed = step
            if first:
                crossed = me ^ step ^ expert_of(refs[0], me, mine, replica, sizes)
            origin = partner_of("tp", mine, -crossed, count)
            start = pl.multiple_of(origin * hidden + offset, 128)
            copies.append(pltpu.make_async_copy(ins[step], out.at[:, pl.ds(start, width)], sems.at[step]))
        for copy in copies:
            copy.start()
        for copy in copies:
            copy.wait()

    return pl.pallas_call(
        kernel,
        in_specs=[SCALARS] * len(table) + [WHOLE] * count + [ANY] * len(saved),
        out_specs=ANY,
        out_shape=jax.ShapeDtypeStruct((block_rows, count * hidden), pieces[0].dtype),
        scratch_shapes=[pltpu.SemaphoreType.DMA((count,))],
        input_output_aliases={len(table) + count: 0} if saved else {},
        compiler_params=PARAMS,
        name="place",
    )(*table, *in_vmem(pieces), *saved)


def exchange(pieces, axis, last):
    count = len(pieces)
    moved = {0: pieces[0]}
    for step in steps_of(axis, count, last):
        pairs = [(index, partner_of(axis, index, step, count)) for index in range(count)]
        moved[step] = lax.ppermute(pieces[step], axis, pairs)
    return [moved[step] for step in range(count)]


def local(down_weight, owned_span):
    weight = pltpu.with_memory_space_constraint(down_weight[0], pltpu.HBM)
    hidden = weight.shape[0]
    owned = pltpu.with_memory_space_constraint(jnp.transpose(owned_span, (0, 2, 1)), pltpu.HBM)
    sizes = tuple(lax.axis_size(name) for name in ("ep", "tp", "dp"))
    chunks, order = plan_of(hidden, weight.shape[1] // sizes[1])

    moved = {}
    saved = []
    for stage, chunk in order:
        first = chunk in TP_FIRST
        offset, width = chunks[chunk]
        if stage == "A":
            sent = pick_rows(weight, owned, sizes, first, offset, width)
        elif stage == "H":
            sent = moved[chunk]
        elif stage == "B":
            sent = choose(moved[chunk], owned, sizes, first)
        else:
            saved = [place(saved, moved[chunk], owned, sizes, first, offset, hidden)]
            continue
        moved[chunk] = exchange(sent, axis_of(stage, chunk), chunk == order[-1][1])
    return saved[0][None, None]


def solution(mesh):
    step = jax.shard_map(
        local,
        mesh=mesh,
        in_specs=(P("ep", "tp", "dp"), P()),
        out_specs=P("ep", "tp", "dp", None),
        check_vma=False,
    )

    def save(down_weight, owned_span):
        sizes = mesh.shape
        hidden = down_weight.shape[1] // sizes["tp"]
        block_rows = down_weight.shape[2] // (sizes["dp"] * sizes["tp"])
        _, _ = plan_of(hidden, block_rows)
        return step(down_weight, owned_span)

    return save
```

```python
import jax
import jax.numpy as jnp
from jax import lax
from jax.experimental import pallas as pl
from jax.experimental.pallas import tpu as pltpu
from jax.sharding import PartitionSpec as P


SHARES = {"X": 1, "Y": 3, "0": 2, "1": 4, "2": 6, "3": 8, "4": 6, "5": 2}
TP_FIRST = "XY"
ORDER = (
    "AX", "AY", "A0", "A1", "B0", "HX", "A2", "B1", "HY", "A3", "C0", "B2", "A4",
    "BX", "C1", "BY", "A5", "B3", "B4", "B5", "C2", "CX", "CY", "C3", "C4", "C5",
)
WORTH_CHUNKS = 1 << 19
ANY = pl.BlockSpec(memory_space=pl.ANY)
SCALARS = pl.BlockSpec(memory_space=pltpu.SMEM)
PARAMS = pltpu.CompilerParams(vmem_limit_bytes=8 << 20)
WHOLE = pl.BlockSpec(memory_space=pltpu.VMEM)


def position():
    return lax.axis_index("ep"), lax.axis_index("tp"), lax.axis_index("dp")


def expert_of(owned, row, column, replica, sizes):
    return lax.div(owned[row, replica, column], sizes[1] * sizes[2])


def span_of(owned, expert, row, column, replica, sizes):
    span = owned[row, replica, column] - (expert * sizes[2] + replica) * sizes[1]
    return jnp.where((span >= 0) & (span < sizes[1]), span, 0)


def tile_of(offset, width):
    return 256 if offset % 256 == 0 and width % 256 == 0 else 128


def plan_of(hidden, block_rows):
    columns = hidden // 128
    if hidden * block_rows < WORTH_CHUNKS or columns < len(SHARES):
        return {"0": (0, hidden)}, ("A0", "B0", "C0")
    total = sum(SHARES.values())
    edges, done = [0], 0
    for left, share in zip(reversed(range(len(SHARES))), SHARES.values()):
        done += share
        edges.append(max(edges[-1] + 1, min(done * columns // total, columns - left)))
    return {chunk: (low * 128, (high - low) * 128) for chunk, low, high in zip(SHARES, edges, edges[1:])}, ORDER


def axis_of(stage, chunk):
    if stage == "A":
        return "tp" if chunk in TP_FIRST else "ep"
    if stage == "B":
        return "ep" if chunk in TP_FIRST else "tp"
    return "ep" if stage == "H" else None


def steps_of(axis, count, last):
    steps = list(range(1, count))
    if axis == "tp" and not last:
        steps.insert(0, steps.pop(count // 2 - 1))
    return steps


def partner_of(axis, index, step, count):
    if axis == "ep":
        return index ^ abs(step)
    rank = index
    shift = 1
    while shift < count:
        rank = rank ^ (rank >> shift)
        shift *= 2
    rank = (rank + step) & (count - 1)
    return rank ^ (rank >> 1)


def in_vmem(pieces):
    return [pltpu.with_memory_space_constraint(piece, pltpu.VMEM) for piece in pieces]


def pick_rows(weight, owned, sizes, first, offset, width):
    count = sizes[1]
    tile = tile_of(offset, width)
    rows = weight.shape[1]
    block_rows = rows // count
    lanes = block_rows % 128 == 0

    def kernel(owned_ref, weight_ref, *refs):
        outs, turned = refs[:count], refs[count:]
        me, mine, replica = position()
        if not lanes:
            turned[0][...] = weight_ref[...].T
        columns = pl.ds(pl.multiple_of(pl.program_id(0) * tile, 128), tile)
        for step, out in enumerate(outs):
            row, column = me ^ step, partner_of("tp", mine, step, count)
            owners = [(line, column) if first else (row, line) for line in range(count)]
            span = sum(span_of(owned_ref, me, row, column, replica, sizes) for row, column in owners)
            if lanes:
                out[:, columns] = weight_ref[:, pl.ds(pl.multiple_of(span * block_rows, 128), block_rows)].T
            else:
                out[:, columns] = turned[0][pl.ds(pl.multiple_of(span * block_rows, 16), block_rows), :]

    return pl.pallas_call(
        kernel,
        grid=(width // tile,),
        in_specs=[SCALARS, pl.BlockSpec((tile, rows), lambda step: (offset // tile + step, 0))],
        out_specs=[WHOLE] * count,
        out_shape=[pltpu.VMEM((block_rows, width), weight.dtype)] * count,
        scratch_shapes=[] if lanes else [pltpu.VMEM((rows, tile), weight.dtype)],
        compiler_params=PARAMS,
        name="pick_rows",
    )(owned, weight)


def choose(pieces, owned, sizes, first):
    count = len(pieces)

    def kernel(owned_ref, *refs):
        ins, outs = refs[:count], refs[count:]
        me, mine, replica = position()
        for step in range(count):
            row, column = (me ^ step, mine) if first else (me, partner_of("tp", mine, step, count))
            pick = expert_of(owned_ref, row, column, replica, sizes) ^ me
            for source in range(count):
                @pl.when(pick == source)
                def _():
                    outs[step][...] = ins[source][...]

    return pl.pallas_call(
        kernel,
        in_specs=[SCALARS] + [WHOLE] * count,
        out_specs=[WHOLE] * count,
        out_shape=[pltpu.VMEM(piece.shape, piece.dtype) for piece in pieces],
        compiler_params=PARAMS,
        name="choose",
    )(owned, *in_vmem(pieces))


def place(saved, pieces, owned, sizes, first, offset, hidden):
    count = len(pieces)
    block_rows, width = pieces[0].shape

    table = [owned] if first else []

    def kernel(*refs):
        ins, out, sems = refs[len(table):len(table) + count], refs[-2], refs[-1]
        me, mine, replica = position()
        copies = []
        for step in range(count):
            crossed = step
            if first:
                crossed = me ^ step ^ expert_of(refs[0], me, mine, replica, sizes)
            origin = partner_of("tp", mine, -crossed, count)
            start = pl.multiple_of(origin * hidden + offset, 128)
            copies.append(pltpu.make_async_copy(ins[step], out.at[:, pl.ds(start, width)], sems.at[step]))
        for copy in copies:
            copy.start()
        for copy in copies:
            copy.wait()

    return pl.pallas_call(
        kernel,
        in_specs=[SCALARS] * len(table) + [WHOLE] * count + [ANY] * len(saved),
        out_specs=ANY,
        out_shape=jax.ShapeDtypeStruct((block_rows, count * hidden), pieces[0].dtype),
        scratch_shapes=[pltpu.SemaphoreType.DMA((count,))],
        input_output_aliases={len(table) + count: 0} if saved else {},
        compiler_params=PARAMS,
        name="place",
    )(*table, *in_vmem(pieces), *saved)


def exchange(pieces, axis, last):
    count = len(pieces)
    moved = {0: pieces[0]}
    for step in steps_of(axis, count, last):
        pairs = [(index, partner_of(axis, index, step, count)) for index in range(count)]
        moved[step] = lax.ppermute(pieces[step], axis, pairs)
    return [moved[step] for step in range(count)]


def local(down_weight, owned_span):
    weight = pltpu.with_memory_space_constraint(down_weight[0], pltpu.HBM)
    hidden = weight.shape[0]
    owned = pltpu.with_memory_space_constraint(jnp.transpose(owned_span, (0, 2, 1)), pltpu.HBM)
    sizes = tuple(lax.axis_size(name) for name in ("ep", "tp", "dp"))
    chunks, order = plan_of(hidden, weight.shape[1] // sizes[1])

    moved = {}
    saved = []
    for stage, chunk in order:
        first = chunk in TP_FIRST
        offset, width = chunks[chunk]
        if stage == "A":
            sent = pick_rows(weight, owned, sizes, first, offset, width)
        elif stage == "H":
            sent = moved[chunk]
        elif stage == "B":
            sent = choose(moved[chunk], owned, sizes, first)
        else:
            saved = [place(saved, moved[chunk], owned, sizes, first, offset, hidden)]
            continue
        moved[chunk] = exchange(sent, axis_of(stage, chunk), chunk == order[-1][1])
    return saved[0][None, None]


def solution(mesh):
    step = jax.shard_map(
        local,
        mesh=mesh,
        in_specs=(P("ep", "tp", "dp"), P()),
        out_specs=P("ep", "tp", "dp", None),
        check_vma=False,
    )

    def save(down_weight, owned_span):
        sizes = mesh.shape
        hidden = down_weight.shape[1] // sizes["tp"]
        block_rows = down_weight.shape[2] // (sizes["dp"] * sizes["tp"])
        _, _ = plan_of(hidden, block_rows)
        return step(down_weight, owned_span)

    return save
```

```python
import jax
import jax.numpy as jnp
from jax import lax
from jax.experimental import pallas as pl
from jax.experimental.pallas import tpu as pltpu
from jax.sharding import PartitionSpec as P


SHARES = {"X": 1, "Y": 3, "0": 2, "1": 4, "2": 6, "3": 8, "4": 6, "5": 2}
TP_FIRST = "XY"
ORDER = (
    "AX", "AY", "A0", "A1", "B0", "HX", "A2", "B1", "HY", "A3", "C0", "B2", "A4",
    "BX", "C1", "BY", "A5", "B3", "B4", "B5", "C2", "CX", "CY", "C3", "C4", "C5", "D5",
)
WORTH_CHUNKS = 1 << 19
ANY = pl.BlockSpec(memory_space=pl.ANY)
SCALARS = pl.BlockSpec(memory_space=pltpu.SMEM)
PARAMS = pltpu.CompilerParams(vmem_limit_bytes=8 << 20)
WHOLE = pl.BlockSpec(memory_space=pltpu.VMEM)


def position():
    return lax.axis_index("ep"), lax.axis_index("tp"), lax.axis_index("dp")


def expert_of(owned, row, column, replica, sizes):
    return lax.div(owned[row, replica, column], sizes[1] * sizes[2])


def span_of(owned, expert, row, column, replica, sizes):
    span = owned[row, replica, column] - (expert * sizes[2] + replica) * sizes[1]
    return jnp.where((span >= 0) & (span < sizes[1]), span, 0)


def tile_of(offset, width):
    return 256 if offset % 256 == 0 and width % 256 == 0 else 128


def plan_of(hidden, block_rows):
    columns = hidden // 128
    if hidden * block_rows < WORTH_CHUNKS or columns < len(SHARES):
        return {"0": (0, hidden)}, ("A0", "B0", "C0")
    total = sum(SHARES.values())
    edges, done = [0], 0
    for left, share in zip(reversed(range(len(SHARES))), SHARES.values()):
        done += share
        edges.append(max(edges[-1] + 1, min(done * columns // total, columns - left)))
    return {chunk: (low * 128, (high - low) * 128) for chunk, low, high in zip(SHARES, edges, edges[1:])}, ORDER


def axis_of(stage, chunk):
    if stage == "A":
        return "tp" if chunk in TP_FIRST else "ep"
    if stage == "B":
        return "ep" if chunk in TP_FIRST else "tp"
    return "ep" if stage == "H" else None


def steps_of(axis, count, last):
    steps = list(range(1, count))
    if axis == "tp" and not last:
        steps.insert(0, steps.pop(count // 2 - 1))
    return steps


def partner_of(axis, index, step, count):
    if axis == "ep":
        return index ^ abs(step)
    rank = index
    shift = 1
    while shift < count:
        rank = rank ^ (rank >> shift)
        shift *= 2
    rank = (rank + step) & (count - 1)
    return rank ^ (rank >> 1)


def in_vmem(pieces):
    return [pltpu.with_memory_space_constraint(piece, pltpu.VMEM) for piece in pieces]


def pick_rows(weight, owned, sizes, first, offset, width):
    count = sizes[1]
    tile = tile_of(offset, width)
    rows = weight.shape[1]
    block_rows = rows // count

    def kernel(owned_ref, weight_ref, *refs):
        outs, turned = refs[:-1], refs[-1]
        me, mine, replica = position()
        turned[...] = weight_ref[...].T
        columns = pl.ds(pl.multiple_of(pl.program_id(0) * tile, 128), tile)
        for step, out in enumerate(outs):
            row, column = me ^ step, partner_of("tp", mine, step, count)
            owners = [(line, column) if first else (row, line) for line in range(count)]
            span = sum(span_of(owned_ref, me, row, column, replica, sizes) for row, column in owners)
            out[:, columns] = turned[pl.ds(pl.multiple_of(span * block_rows, 16), block_rows), :]

    return pl.pallas_call(
        kernel,
        grid=(width // tile,),
        in_specs=[SCALARS, pl.BlockSpec((tile, rows), lambda step: (offset // tile + step, 0))],
        out_specs=[WHOLE] * count,
        out_shape=[pltpu.VMEM((block_rows, width), weight.dtype)] * count,
        scratch_shapes=[pltpu.VMEM((rows, tile), weight.dtype)],
        compiler_params=PARAMS,
        name="pick_rows",
    )(owned, weight)


def choose(pieces, owned, sizes, first):
    count = len(pieces)

    def kernel(owned_ref, *refs):
        ins, outs = refs[:count], refs[count:]
        me, mine, replica = position()
        for step in range(count):
            row, column = (me ^ step, mine) if first else (me, partner_of("tp", mine, step, count))
            pick = expert_of(owned_ref, row, column, replica, sizes) ^ me
            for source in range(count):
                @pl.when(pick == source)
                def _():
                    outs[step][...] = ins[source][...]

    return pl.pallas_call(
        kernel,
        in_specs=[SCALARS] + [WHOLE] * count,
        out_specs=[WHOLE] * count,
        out_shape=[pltpu.VMEM(piece.shape, piece.dtype) for piece in pieces],
        compiler_params=PARAMS,
        name="choose",
    )(owned, *in_vmem(pieces))


def place(saved, landed, owned, sizes, first, offset, hidden):
    steps, pieces = tuple(landed), tuple(landed.values())
    count = len(pieces)
    block_rows, width = pieces[0].shape

    table = [owned] if first else []

    def kernel(*refs):
        ins, out, sems = refs[len(table):len(table) + count], refs[-2], refs[-1]
        me, mine, replica = position()
        copies = []
        for slot, step in enumerate(steps):
            crossed = step
            if first:
                crossed = me ^ step ^ expert_of(refs[0], me, mine, replica, sizes)
            origin = partner_of("tp", mine, -crossed, sizes[1])
            start = pl.multiple_of(origin * hidden + offset, 128)
            copies.append(pltpu.make_async_copy(ins[slot], out.at[:, pl.ds(start, width)], sems.at[slot]))
        for copy in copies:
            copy.start()
        for copy in copies:
            copy.wait()

    return pl.pallas_call(
        kernel,
        in_specs=[SCALARS] * len(table) + [WHOLE] * count + [ANY] * len(saved),
        out_specs=ANY,
        out_shape=jax.ShapeDtypeStruct((block_rows, sizes[1] * hidden), pieces[0].dtype),
        scratch_shapes=[pltpu.SemaphoreType.DMA((count,))],
        input_output_aliases={len(table) + count: 0} if saved else {},
        compiler_params=PARAMS,
        name="place",
    )(*table, *in_vmem(pieces), *saved)


def exchange(pieces, axis, last):
    count = len(pieces)
    moved = {0: pieces[0]}
    for step in steps_of(axis, count, last):
        pairs = [(index, partner_of(axis, index, step, count)) for index in range(count)]
        moved[step] = lax.ppermute(pieces[step], axis, pairs)
    return [moved[step] for step in range(count)]


def local(down_weight, owned_span):
    weight = pltpu.with_memory_space_constraint(down_weight[0], pltpu.HBM)
    hidden = weight.shape[0]
    owned = pltpu.with_memory_space_constraint(jnp.transpose(owned_span, (0, 2, 1)), pltpu.HBM)
    sizes = tuple(lax.axis_size(name) for name in ("ep", "tp", "dp"))
    chunks, order = plan_of(hidden, weight.shape[1] // sizes[1])

    moved = {}
    saved = []
    for stage, chunk in order:
        first = chunk in TP_FIRST
        offset, width = chunks[chunk]
        if stage == "A":
            sent = pick_rows(weight, owned, sizes, first, offset, width)
        elif stage == "H":
            sent = moved[chunk]
        elif stage == "B":
            sent = choose(moved[chunk], owned, sizes, first)
        else:
            early = sizes[1] // 2 if "D" + chunk in order else sizes[1]
            landed = list(enumerate(moved[chunk]))
            landed = landed[early:] if stage == "D" else landed[:early]
            saved = [place(saved, dict(landed), owned, sizes, first, offset, hidden)]
            continue
        moved[chunk] = exchange(sent, axis_of(stage, chunk), chunk == order[-1][1])
    return saved[0][None, None]


def solution(mesh):
    step = jax.shard_map(
        local,
        mesh=mesh,
        in_specs=(P("ep", "tp", "dp"), P()),
        out_specs=P("ep", "tp", "dp", None),
        check_vma=False,
    )

    def save(down_weight, owned_span):
        sizes = mesh.shape
        hidden = down_weight.shape[1] // sizes["tp"]
        block_rows = down_weight.shape[2] // (sizes["dp"] * sizes["tp"])
        _, _ = plan_of(hidden, block_rows)
        return step(down_weight, owned_span)

    return save
```

```python
import jax
import jax.numpy as jnp
from jax import lax
from jax.experimental import pallas as pl
from jax.experimental.pallas import tpu as pltpu
from jax.sharding import PartitionSpec as P


SHARES = {"X": 1, "Y": 3, "0": 2, "1": 4, "2": 6, "3": 8, "4": 6, "5": 2}
TP_FIRST = "XY"
ORDER = (
    "AX", "AY", "A0", "A1", "B0", "HX", "A2", "B1", "HY", "A3", "C0", "B2", "A4",
    "BX", "C1", "BY", "A5", "B3", "B4", "B5", "C2", "CX", "CY", "C3", "C4", "C5", "D5",
)
WORTH_CHUNKS = 1 << 19
ANY = pl.BlockSpec(memory_space=pl.ANY)
SCALARS = pl.BlockSpec(memory_space=pltpu.SMEM)
PARAMS = pltpu.CompilerParams(vmem_limit_bytes=8 << 20)
WHOLE = pl.BlockSpec(memory_space=pltpu.VMEM)


def position():
    return lax.axis_index("ep"), lax.axis_index("tp"), lax.axis_index("dp")


def expert_of(owned, row, column, replica, sizes):
    return lax.div(owned[row, replica, column], sizes[1] * sizes[2])


def span_of(owned, expert, row, column, replica, sizes):
    span = owned[row, replica, column] - (expert * sizes[2] + replica) * sizes[1]
    return jnp.where((span >= 0) & (span < sizes[1]), span, 0)


def tile_of(offset, width):
    return 256 if offset % 256 == 0 and width % 256 == 0 else 128


def plan_of(hidden, block_rows):
    columns = hidden // 128
    if hidden * block_rows < WORTH_CHUNKS or columns < len(SHARES):
        return {"0": (0, hidden)}, ("A0", "B0", "C0")
    total = sum(SHARES.values())
    edges, done = [0], 0
    for left, share in zip(reversed(range(len(SHARES))), SHARES.values()):
        done += share
        edges.append(max(edges[-1] + 1, min(done * columns // total, columns - left)))
    return {chunk: (low * 128, (high - low) * 128) for chunk, low, high in zip(SHARES, edges, edges[1:])}, ORDER


def axis_of(stage, chunk):
    if stage == "A":
        return "tp" if chunk in TP_FIRST else "ep"
    if stage == "B":
        return "ep" if chunk in TP_FIRST else "tp"
    return "ep" if stage == "H" else None


def steps_of(axis, count, last):
    steps = list(range(1, count))
    if axis == "tp" and not last:
        steps.insert(0, steps.pop(count // 2 - 1))
    return steps


def partner_of(axis, index, step, count):
    if axis == "ep":
        return index ^ abs(step)
    rank = index
    shift = 1
    while shift < count:
        rank = rank ^ (rank >> shift)
        shift *= 2
    rank = (rank + step) & (count - 1)
    return rank ^ (rank >> 1)


def in_vmem(pieces):
    return [pltpu.with_memory_space_constraint(piece, pltpu.VMEM) for piece in pieces]


def pick_rows(weight, owned, sizes, first, offset, width):
    count = sizes[1]
    tile = tile_of(offset, width)
    rows = weight.shape[1]
    block_rows = rows // count
    lanes = block_rows % 128 == 0

    def kernel(owned_ref, weight_ref, *refs):
        outs, turned = refs[:count], refs[count:]
        me, mine, replica = position()
        if not lanes:
            turned[0][...] = weight_ref[...].T
        columns = pl.ds(pl.multiple_of(pl.program_id(0) * tile, 128), tile)
        for step, out in enumerate(outs):
            row, column = me ^ step, partner_of("tp", mine, step, count)
            owners = [(line, column) if first else (row, line) for line in range(count)]
            span = sum(span_of(owned_ref, me, row, column, replica, sizes) for row, column in owners)
            if lanes:
                out[:, columns] = weight_ref[:, pl.ds(pl.multiple_of(span * block_rows, 128), block_rows)].T
            else:
                out[:, columns] = turned[0][pl.ds(pl.multiple_of(span * block_rows, 16), block_rows), :]

    return pl.pallas_call(
        kernel,
        grid=(width // tile,),
        in_specs=[SCALARS, pl.BlockSpec((tile, rows), lambda step: (offset // tile + step, 0))],
        out_specs=[WHOLE] * count,
        out_shape=[pltpu.VMEM((block_rows, width), weight.dtype)] * count,
        scratch_shapes=[] if lanes else [pltpu.VMEM((rows, tile), weight.dtype)],
        compiler_params=PARAMS,
        name="pick_rows",
    )(owned, weight)


def choose(pieces, owned, sizes, first):
    count = len(pieces)

    def kernel(owned_ref, *refs):
        ins, outs = refs[:count], refs[count:]
        me, mine, replica = position()
        for step in range(count):
            row, column = (me ^ step, mine) if first else (me, partner_of("tp", mine, step, count))
            pick = expert_of(owned_ref, row, column, replica, sizes) ^ me
            for source in range(count):
                @pl.when(pick == source)
                def _():
                    outs[step][...] = ins[source][...]

    return pl.pallas_call(
        kernel,
        in_specs=[SCALARS] + [WHOLE] * count,
        out_specs=[WHOLE] * count,
        out_shape=[pltpu.VMEM(piece.shape, piece.dtype) for piece in pieces],
        compiler_params=PARAMS,
        name="choose",
    )(owned, *in_vmem(pieces))


def place(saved, landed, owned, sizes, first, offset, hidden):
    steps, pieces = tuple(landed), tuple(landed.values())
    count = len(pieces)
    block_rows, width = pieces[0].shape

    table = [owned] if first else []

    def kernel(*refs):
        ins, out, sems = refs[len(table):len(table) + count], refs[-2], refs[-1]
        me, mine, replica = position()
        copies = []
        for slot, step in enumerate(steps):
            crossed = step
            if first:
                crossed = me ^ step ^ expert_of(refs[0], me, mine, replica, sizes)
            origin = partner_of("tp", mine, -crossed, sizes[1])
            start = pl.multiple_of(origin * hidden + offset, 128)
            copies.append(pltpu.make_async_copy(ins[slot], out.at[:, pl.ds(start, width)], sems.at[slot]))
        for copy in copies:
            copy.start()
        for copy in copies:
            copy.wait()

    return pl.pallas_call(
        kernel,
        in_specs=[SCALARS] * len(table) + [WHOLE] * count + [ANY] * len(saved),
        out_specs=ANY,
        out_shape=jax.ShapeDtypeStruct((block_rows, sizes[1] * hidden), pieces[0].dtype),
        scratch_shapes=[pltpu.SemaphoreType.DMA((count,))],
        input_output_aliases={len(table) + count: 0} if saved else {},
        compiler_params=PARAMS,
        name="place",
    )(*table, *in_vmem(pieces), *saved)


def exchange(pieces, axis, last):
    count = len(pieces)
    moved = {0: pieces[0]}
    for step in steps_of(axis, count, last):
        pairs = [(index, partner_of(axis, index, step, count)) for index in range(count)]
        moved[step] = lax.ppermute(pieces[step], axis, pairs)
    return [moved[step] for step in range(count)]


def local(down_weight, owned_span):
    weight = pltpu.with_memory_space_constraint(down_weight[0], pltpu.HBM)
    hidden = weight.shape[0]
    owned = pltpu.with_memory_space_constraint(jnp.transpose(owned_span, (0, 2, 1)), pltpu.HBM)
    sizes = tuple(lax.axis_size(name) for name in ("ep", "tp", "dp"))
    chunks, order = plan_of(hidden, weight.shape[1] // sizes[1])

    moved = {}
    saved = []
    for stage, chunk in order:
        first = chunk in TP_FIRST
        offset, width = chunks[chunk]
        if stage == "A":
            sent = pick_rows(weight, owned, sizes, first, offset, width)
        elif stage == "H":
            sent = moved[chunk]
        elif stage == "B":
            sent = choose(moved[chunk], owned, sizes, first)
        else:
            early = sizes[1] // 2 if "D" + chunk in order else sizes[1]
            landed = list(enumerate(moved[chunk]))
            landed = landed[early:] if stage == "D" else landed[:early]
            saved = [place(saved, dict(landed), owned, sizes, first, offset, hidden)]
            continue
        moved[chunk] = exchange(sent, axis_of(stage, chunk), chunk == order[-1][1])
    return saved[0][None, None]


def solution(mesh):
    step = jax.shard_map(
        local,
        mesh=mesh,
        in_specs=(P("ep", "tp", "dp"), P()),
        out_specs=P("ep", "tp", "dp", None),
        check_vma=False,
    )

    def save(down_weight, owned_span):
        sizes = mesh.shape
        hidden = down_weight.shape[1] // sizes["tp"]
        block_rows = down_weight.shape[2] // (sizes["dp"] * sizes["tp"])
        _, _ = plan_of(hidden, block_rows)
        return step(down_weight, owned_span)

    return save
```
